1024 devices in a mesh: rep: 8 (over x_hi, core), dp: 16 (over z, x_lo), tp: 8 (over y).
Axes of the slice: x: 8 (x_hi: 4, x_lo: 2; x = x_hi * 2 + x_lo), y: 8, z: 8, core: 2. Of those that a mesh axis runs over, the one named last changes fastest.
Arguments:
- hidden: bfloat16 [8, 512, 14336], P('rep', None, 'tp'), may hold values from -6 to 6
- down_weight: bfloat16 [14336, 8192], P('tp', 'dp'), may hold values from -0.046875 to 0.046875
- out_grad: bfloat16 [8, 512, 8192], P('rep', 'tp', 'dp'), may hold values from -6 to 6
- pseudo_grad: bfloat16 [8, 14336, 8192], P('rep', 'tp', 'dp'), may hold values from -6 to 6
- momentum: float32 [14336, 8192], P(('tp', 'rep'), 'dp'), may hold values from -6 to 6
Outputs:
- layer_out: bfloat16 [8, 512, 8192], P('rep', 'tp', 'dp')
- hidden_grad: bfloat16 [8, 512, 14336], P('rep', 'dp', 'tp')
- new_momentum: float32 [14336, 8192], P(('tp', 'rep'), 'dp')
- outer_step: bfloat16 [14336, 8192], P('tp', 'dp')
The draws below stay inside these ranges and needn't reach their ends.
All inputs are finite; a program needn't handle non-finite values.
Results may differ from the reference program's by a relative error of at most 0.017.
Values may be sent and summed in bfloat16 or wider, within the bound.
A program may use at most 64 MiB of HBM per device.

```python
import jax
import jax.numpy as jnp
from jax import lax

D = 8192
FF = 14336
TOKENS = 512
N_REP = 8
N_DP = 16
N_TP = 8


def block_scale(key, extent, cuts, low, largest):
    gain = 1.0
    for axis_at, parts in cuts:
        heights = jax.random.uniform(jax.random.fold_in(jax.random.fold_in(key, 6), axis_at), (parts,), jnp.float32, low / len(cuts), largest / len(cuts))
        gain = gain * jnp.repeat(jnp.exp(heights), extent[axis_at] // parts).reshape((-1,) + (1,) * (len(extent) - 1 - axis_at))
    return gain


def bell_draw(rng, dims, spread, reach, cuts=(), kind=jnp.bfloat16):
    level = block_scale(rng, dims, cuts, -0.22, 0.18) if cuts else 1.0
    array = jax.random.normal(rng, dims, jnp.float32) * spread * level
    return jnp.minimum(jnp.maximum(array, -reach), reach).astype(kind)


def setup_inputs(seed: int = 0) -> dict:
    key_list = jax.random.split(jax.random.key(seed), 6)
    return {
        "hidden": bell_draw(key_list[0], (N_REP, TOKENS, FF), 1.0, 6.0, ((0, 8), (2, 8))),
        "down_weight": bell_draw(key_list[1], (FF, D), FF ** -0.5, 0.046875, ((0, 8), (1, 16))),
        "out_grad": bell_draw(key_list[2], (N_REP, TOKENS, D), 1.0, 6.0, ((0, 8), (1, 8), (2, 16))),
        "pseudo_grad": bell_draw(key_list[3], (N_REP, FF, D), 1.0, 6.0, ((0, 8), (1, 8), (2, 16))),
        "momentum": bell_draw(key_list[4], (FF, D), 1.0, 6.0, ((0, 64), (1, 16)), jnp.float32),
    }


outer_rate = 0.7
momentum_rate = 0.9


def reference(hidden, down_weight, out_grad, pseudo_grad, momentum):
    hidden_width = FF // N_TP
    model_width = D // N_DP
    weight_tp = down_weight.reshape(N_TP, hidden_width, D)
    weight_dp = jnp.transpose(down_weight.reshape(FF, N_DP, model_width), (1, 0, 2))

    def forward_block(paired):
        return jnp.dot(paired[0], paired[1], preferred_element_type=jnp.float32).astype(jnp.bfloat16)

    def backward_block(paired):
        product = lax.dot_general(paired[0], paired[1], (((1,), (1,)), ((), ())), preferred_element_type=jnp.float32)
        return product.astype(jnp.bfloat16)

    def one_replica(paired):
        token_rows = paired[0]
        grad_rows = paired[1]
        rows_tp = jnp.transpose(token_rows.reshape(TOKENS, N_TP, hidden_width), (1, 0, 2))
        partial_out = lax.map(forward_block, (rows_tp, weight_tp))
        layer = jnp.sum(partial_out.astype(jnp.float32), axis=0).astype(jnp.bfloat16)
        grads_dp = jnp.transpose(grad_rows.reshape(TOKENS, N_DP, model_width), (1, 0, 2))
        partial_back = lax.map(backward_block, (grads_dp, weight_dp))
        back = jnp.sum(partial_back.astype(jnp.float32), axis=0).astype(jnp.bfloat16)
        return layer, back

    layer_out, hidden_grad = lax.map(one_replica, (hidden, out_grad))

    def accumulate(index, running_sum):
        return running_sum + pseudo_grad[index].astype(jnp.float32)

    totals = lax.fori_loop(0, N_REP, accumulate, jnp.zeros((FF, D), jnp.float32))
    average = totals / N_REP
    new_momentum = momentum_rate * momentum + average
    outer_step = (outer_rate * (average + momentum_rate * new_momentum)).astype(jnp.bfloat16)
    return layer_out, hidden_grad, new_momentum, outer_step
```

```python
import functools

import jax
import jax.numpy as jnp
from jax import lax
from jax.experimental import pallas as pl
from jax.experimental.pallas import tpu as pltpu
from jax.sharding import PartitionSpec as P

outer_rate = 0.7
momentum_rate = 0.9
MESH = pl.DeviceIdType.MESH
F32, BF16 = jnp.float32, jnp.bfloat16
PIECES_X = 2
PIECES_Z = 2


def arm(n, sign, half):
    return n // 2 - (0 if (sign > 0) == (half == 0) else 1)


def ring_items(n, pieces):
    return [
        (s, h, d, c)
        for s in (1, -1)
        for h in (0, 1)
        for d in range(1, arm(n, s, h) + 1)
        for c in range(pieces)
    ]


def gather_plan(n):
    if n == 8:
        near = [(2, 0, 2), (-2, 0, 2), (1, 0, 2), (-1, 0, 2)]
        far = [(3, 2, 2), (-3, -2, 2), (4, 2, 0), (-4, -2, 1)]
        return near, far
    return [(o, 0, 2) for o in range(1, n)], []


def kernel(
    n_rep, n_dp, n_tp,
    hid, w, og, pg, mom,
    lay_o, hg_o, nm_o, out_o,
    hid_v, w_v, og_v, pgo, pgm, mom_v, dd, xr, outv, nm_v,
    po, lrecv, lay_v, part, brecv, fin, xs, xrv, hg_v,
    load_sem, dd_sem, rs_sem, ag_sem, pass_sem, put_sem, g_sem, l_sem, b_sem, e_sem, o_sem,
):
    n_x, n_z, n_y = n_rep // 2, n_dp // 2, n_tp
    rep, dp, y = lax.axis_index("rep"), lax.axis_index("dp"), lax.axis_index("tp")
    x, core = rep // 2, rep % 2
    z, low = dp // 2, dp % 2
    width = w.shape[1]
    units = w.shape[0]
    shift = n_z // 2 - 1

    def at_x(k):
        return lax.rem(x + k % n_x, n_x)

    def to_x(s):
        return {"rep": 2 * at_x(s) + core}

    def to_z(s):
        return {"dp": 2 * lax.rem(z + s % n_z, n_z) + low}

    def to_y(o):
        return {"tp": lax.rem(y + o % n_y, n_y)}

    partner = {"rep": 2 * x + 1 - core}
    pair = {"dp": 2 * z + 1 - low}

    def remote(src, dst, sems, i, where):
        return pltpu.make_async_remote_copy(
            src_ref=src, dst_ref=dst, send_sem=sems.at[0, i], recv_sem=sems.at[1, i],
            device_id=where, device_id_type=MESH,
        )

    def span(total, pieces, c):
        return pl.ds(c * (total // pieces), total // pieces)

    sent = []

    def go(copy):
        copy.start()
        sent.append(copy)
        return copy

    order_x = sorted(range(n_x), key=lambda k: -min(k, n_x - k))
    slot_me = lax.rem(y + (-shift) % n_z + n_z - z, n_z)
    loads = {}

    def load(name, src, dst):
        loads[name] = pltpu.make_async_copy(src, dst, load_sem.at[len(loads)])
        loads[name].start()

    load("og", og, og_v.at[slot_me])
    for k in order_x:
        load(("o", k), pg.at[2 * at_x(k) + 1 - core], pgo.at[k])
    for k in order_x:
        load(("m", k), pg.at[2 * at_x(k) + core], pgm.at[k])
    load("w", w, w_v)
    load("hid", hid, hid_v)
    load("mom", mom, mom_v)

    peers = [partner, pair]
    peers += [to_x(s) for s in sorted({1 % n_x, -1 % n_x} - {0})]
    peers += [to_z(s) for s in sorted({1 % n_z, -1 % n_z} - {0})]
    peers += [to_y(o) for o in range(1, n_y)]
    barrier = pltpu.get_barrier_semaphore()
    for where in peers:
        pl.semaphore_signal(barrier, inc=1, device_id=where, device_id_type=MESH)
    pl.semaphore_wait(barrier, len(peers))

    near, far = gather_plan(n_y)
    g_index = {o: i for i, (o, _, _) in enumerate(near + far)}
    gathers = {}
    half_rows = og.shape[0] // 2

    def gather(o, relay, rows):
        slot = lax.rem(slot_me + (-relay) % n_z, n_z)
        ref = og_v.at[slot]
        if rows < 2:
            ref = ref.at[pl.ds(rows * half_rows, half_rows)]
        gathers[o] = go(remote(ref, ref, g_sem, g_index[o], to_y(o - relay)))

    loads["og"].wait()
    for o, relay, rows in near:
        gather(o, relay, rows)
    swaps = {}
    for k in order_x:
        loads["o", k].wait()
        swaps[k] = go(remote(pgo.at[k], dd.at[k], dd_sem, k, partner))

    ready = set()

    def have(k):
        if k not in ready:
            ready.add(k)
            swaps[k].wait_recv()
            loads["m", k].wait()

    x_items = ring_items(n_x, PIECES_X)
    x_index = {key: i for i, key in enumerate(x_items)}
    rs = {}

    def sign_at(s):
        return 0 if s > 0 else 1

    def rs_send(s, h, d, c):
        k = (s * d) % n_x
        cols = span(width, PIECES_X, c)
        total = pgm[k, h, :, cols].astype(F32) + dd[k, h, :, cols].astype(F32)
        if d < arm(n_x, s, h):
            rs[s, h, d + 1, c].wait_recv()
            total = total + xr[sign_at(s), h, d, :, cols].astype(F32)
        dd[k, h, :, cols] = total.astype(BF16)
        rs[s, h, d, c] = go(
            remote(dd.at[k, h, :, cols], xr.at[sign_at(s), h, d - 1, :, cols], rs_sem, x_index[s, h, d, c], to_x(s))
        )

    ag = {}

    def ag_send(s, h, d, c):
        cols = span(width, PIECES_X, c)
        ag[s, h, d, c] = go(
            remote(
                outv.at[(-s * (d - 1)) % n_x, h, :, cols], outv.at[(-s * d) % n_x, h, :, cols],
                ag_sem, x_index[s, h, d, c], to_x(s),
            )
        )

    passed, puts = [], []

    def hand_out(k, h, c):
        cols = span(width, PIECES_X, c)
        i = (k * 2 + h) * PIECES_X + c
        home = out_o.at[2 * at_x(k) + core, h, :, cols]
        passed.append(go(remote(outv.at[k, h, :, cols], home, pass_sem, i, partner)))
        put = pltpu.make_async_copy(outv.at[k, h, :, cols], home, put_sem.at[i])
        put.start()
        puts.append(put)

    def rs_end(c):
        have(0)
        cols = span(width, PIECES_X, c)
        for h in (0, 1):
            total = pgm[0, h, :, cols].astype(F32) + dd[0, h, :, cols].astype(F32)
            for s in (1, -1):
                if arm(n_x, s, h) >= 1:
                    rs[s, h, 1, c].wait_recv()
                    total = total + xr[sign_at(s), h, 0, :, cols].astype(F32)
            average = total * (1.0 / n_rep)
            new = momentum_rate * mom_v[h, :, cols] + average
            nm_v[h, :, cols] = new
            outv[0, h, :, cols] = (outer_rate * (average + momentum_rate * new)).astype(BF16)
        for far_first in (True, False):
            for s in (1, -1):
                for h in (0, 1):
                    if arm(n_x, s, h) >= 1 and ((s > 0) == (h == 0)) == far_first:
                        ag_send(s, h, 1, c)
        for h in (0, 1):
            hand_out(0, h, c)

    def ag_take(s, h, d, c):
        ag[s, h, d, c].wait_recv()
        if d < arm(n_x, s, h):
            ag_send(s, h, d + 1, c)
        hand_out((-s * d) % n_x, h, c)

    starts = []
    for c in range(PIECES_X):
        for s in (1, -1):
            for h in (0, 1):
                d = arm(n_x, s, h)
                if d >= 1:
                    starts.append((c, -d, s, h, d))
    for c, _, s, h, d in sorted(starts):
        have((s * d) % n_x)
        rs_send(s, h, d, c)

    loads["w"].wait()
    loads["hid"].wait()
    tile = min(256, width)

    @pl.loop(0, width // tile)
    def _(j):
        cols = pl.ds(pl.multiple_of(j * tile, tile), tile)
        block = jnp.dot(hid_v[...], w_v[:, cols], preferred_element_type=F32)
        po[:, :, cols] = block.astype(BF16).reshape(n_y, -1, tile)

    relayed = set()
    for o, relay, rows in far:
        if relay not in relayed:
            relayed.add(relay)
            gathers[relay].wait_recv()
        gather(o, relay, rows)

    def rs_rest(c):
        for d in range(n_x // 2 - 1, 0, -1):
            for s in (1, -1):
                for h in (0, 1):
                    if d < arm(n_x, s, h):
                        rs_send(s, h, d, c)

    for c in range(PIECES_X):
        rs_rest(c)

    for o in gathers:
        if o not in relayed:
            gathers[o].wait_recv()

    outs = []
    exchange = {}
    for o in range(1, n_y):
        exchange[o] = go(remote(po.at[lax.rem(y + o, n_y)], lrecv.at[o - 1], l_sem, o - 1, to_y(o)))

    f_tile = min(256, units)

    def back(a, b):
        @pl.loop(0, units // f_tile)
        def _(j):
            cols = pl.ds(pl.multiple_of(j * f_tile, f_tile), f_tile)
            rows = og_v[pl.ds(a, b - a)].reshape(-1, width)
            block = lax.dot_general(rows, w_v[cols, :], (((1,), (1,)), ((), ())), preferred_element_type=F32)
            part[pl.ds(a, b - a), :, :, cols] = block.astype(BF16).reshape(b - a, 2, -1, f_tile)

    z_items = ring_items(n_z, PIECES_Z)
    z_index = {key: i for i, key in enumerate(z_items)}
    zs = {}

    def z_slot(k):
        return (k - shift) % n_z

    def z_send(s, h, d, c):
        k = z_slot(s * d)
        cols = span(units, PIECES_Z, c)
        if d < arm(n_z, s, h):
            zs[s, h, d + 1, c].wait_recv()
            total = part[k, h, :, cols].astype(F32) + brecv[sign_at(s), h, d, :, cols].astype(F32)
            part[k, h, :, cols] = total.astype(BF16)
        zs[s, h, d, c] = go(
            remote(part.at[k, h, :, cols], brecv.at[sign_at(s), h, d - 1, :, cols], b_sem, z_index[s, h, d, c], to_z(s))
        )

    def z_wave(step, long_arm):
        for c in range(PIECES_Z):
            for s in (1, -1):
                h = 0 if (s > 0) == long_arm else 1
                d = arm(n_z, s, h) - step
                if d >= 1:
                    z_send(s, h, d, c)

    cut = min(3, n_z)
    back(0, cut)
    z_wave(0, True)
    z_wave(0, False)
    if cut < n_z:
        back(cut, n_z)

    ends = {}

    def z_end(c):
        cols = span(units, PIECES_Z, c)
        for h in (0, 1):
            total = part[z_slot(0), h, :, cols].astype(F32)
            for s in (1, -1):
                if arm(n_z, s, h) >= 1:
                    zs[s, h, 1, c].wait_recv()
                    total = total + brecv[sign_at(s), h, 0, :, cols].astype(F32)
            fin[h, :, cols] = total
        xs[:, cols] = fin[1 - low, :, cols].astype(BF16)
        ends[c] = go(remote(xs.at[:, cols], xrv.at[:, cols], e_sem, c, pair))

    def grad_out(c):
        cols = span(units, PIECES_Z, c)
        ends[c].wait_recv()
        hg_v[:, cols] = (fin[low, :, cols] + xrv[:, cols].astype(F32)).astype(BF16)
        put(hg_v.at[:, cols], hg_o.at[:, cols])

    def put(src, dst):
        copy = pltpu.make_async_copy(src, dst, o_sem.at[len(outs)])
        copy.start()
        outs.append(copy)

    def layer_out():
        total = po[y].astype(F32)
        for o in range(1, n_y):
            exchange[o].wait_recv()
            total = total + lrecv[o - 1].astype(F32)
        lay_v[...] = total.astype(BF16)
        put(lay_v, lay_o)

    def takes(d, c):
        for s in (1, -1):
            for h in (0, 1):
                if d <= arm(n_x, s, h):
                    ag_take(s, h, d, c)

    loads["mom"].wait()
    rs_end(0)
    z_wave(1, True)
    for c in range(1, PIECES_X):
        rs_end(c)
    put(nm_v, nm_o)
    z_wave(1, False)
    for c in range(PIECES_X):
        takes(1, c)
        z_wave(2, c == 0)
    for step in range(3, n_z // 2):
        z_wave(step, True)
        z_wave(step, False)
    layer_out()
    for c in range(PIECES_Z):
        z_end(c)
    for d in range(2, n_x // 2 + 1):
        for c in range(PIECES_X):
            takes(d, c)
    for c in range(PIECES_Z):
        grad_out(c)
    for copy in passed:
        copy.wait_recv()
    for copy in sent:
        copy.wait_send()
    for copy in puts + outs:
        copy.wait()


def per_device(sizes, hidden, down_weight, out_grad, pseudo_grad, momentum):
    n_rep, n_dp, n_tp = sizes
    n_x, n_z = n_rep // 2, n_dp // 2
    tokens, units = hidden.shape[1:]
    width = down_weight.shape[1]
    rows = out_grad.shape[1]
    share = momentum.shape[0] // 2
    owned = tokens // n_dp
    far_x, far_z = max(n_x // 2, 1), max(n_z // 2, 1)
    x_copies = max(len(ring_items(n_x, PIECES_X)), 1)
    z_copies = max(len(ring_items(n_z, PIECES_Z)), 1)
    near, far = gather_plan(n_tp)
    any_ref = pl.BlockSpec(memory_space=pl.ANY)
    sem = pltpu.SemaphoreType.DMA
    lay, hg, nm, out = pl.pallas_call(
        functools.partial(kernel, n_rep, n_dp, n_tp),
        out_shape=(
            jax.ShapeDtypeStruct((rows, width), BF16),
            jax.ShapeDtypeStruct((owned, units), BF16),
            jax.ShapeDtypeStruct((2, share, width), F32),
            jax.ShapeDtypeStruct((n_rep, 2, share, width), BF16),
        ),
        in_specs=[any_ref] * 5,
        out_specs=(any_ref,) * 4,
        scratch_shapes=[
            pltpu.VMEM((tokens, units), BF16),
            pltpu.VMEM((units, width), BF16),
            pltpu.VMEM((n_tp, rows, width), BF16),
            pltpu.VMEM((n_x, 2, share, width), BF16),
            pltpu.VMEM((n_x, 2, share, width), BF16),
            pltpu.VMEM((2, share, width), F32),
            pltpu.VMEM((n_x, 2, share, width), BF16),
            pltpu.VMEM((2, 2, far_x, share, width), BF16),
            pltpu.VMEM((n_x, 2, share, width), BF16),
            pltpu.VMEM((2, share, width), F32),
            pltpu.VMEM((n_tp, rows, width), BF16),
            pltpu.VMEM((max(n_tp - 1, 1), rows, width), BF16),
            pltpu.VMEM((rows, width), BF16),
            pltpu.VMEM((n_z, 2, owned, units), BF16),
            pltpu.VMEM((2, 2, far_z, owned, units), BF16),
            pltpu.VMEM((2, owned, units), F32),
            pltpu.VMEM((owned, units), BF16),
            pltpu.VMEM((owned, units), BF16),
            pltpu.VMEM((owned, units), BF16),
            sem((4 + 2 * n_x,)),
            sem((2, n_x)),
            sem((2, x_copies)),
            sem((2, x_copies)),
            sem((2, 2 * n_x * PIECES_X)),
            sem((2 * n_x * PIECES_X,)),
            sem((2, max(len(near + far), 1))),
            sem((2, max(n_tp - 1, 1))),
            sem((2, z_copies)),
            sem((2, PIECES_Z)),
            sem((2 + PIECES_Z,)),
        ],
        compiler_params=pltpu.CompilerParams(collective_id=0, has_side_effects=True),
        name="step",
    )(
        hidden[0],
        down_weight,
        out_grad[0],
        pseudo_grad.reshape(n_rep, 2, share, width),
        momentum.reshape(2, share, width),
    )
    return lay[None], hg[None], nm.reshape(momentum.shape), out.reshape(down_weight.shape)


def solution(mesh):
    sizes = tuple(mesh.shape[axis] for axis in ("rep", "dp", "tp"))
    return jax.shard_map(
        functools.partial(per_device, sizes),
        mesh=mesh,
        in_specs=(
            P("rep", None, "tp"),
            P("tp", "dp"),
            P("rep", "tp", "dp"),
            P("rep", "tp", "dp"),
            P(("tp", "rep"), "dp"),
        ),
        out_specs=(
            P("rep", "tp", "dp"),
            P("rep", "dp", "tp"),
            P(("tp", "rep"), "dp"),
            P("tp", "dp"),
        ),
        check_vma=False,
    )
```

```python
import functools

import jax
import jax.numpy as jnp
from jax import lax
from jax.experimental import pallas as pl
from jax.experimental.pallas import tpu as pltpu
from jax.sharding import PartitionSpec as P

outer_rate = 0.7
momentum_rate = 0.9
MESH = pl.DeviceIdType.MESH
F32, BF16 = jnp.float32, jnp.bfloat16
PIECES_X = 2
PIECES_Z = 2


def arm(n, sign, half):
    return n // 2 - (0 if (sign > 0) == (half == 0) else 1)


def ring_items(n, pieces):
    return [
        (s, h, d, c)
        for s in (1, -1)
        for h in (0, 1)
        for d in range(1, arm(n, s, h) + 1)
        for c in range(pieces)
    ]


def gather_plan(n):
    if n == 8:
        near = [(2, 0, 2), (-2, 0, 2), (1, 0, 2), (-1, 0, 2)]
        far = [(4, 2, 0), (-4, -2, 1), (3, 2, 2), (-3, -2, 2)]
        return near, far
    return [(o, 0, 2) for o in range(1, n)], []


def kernel(
    n_rep, n_dp, n_tp,
    hid, w, og, pg, mom,
    lay_o, hg_o, nm_o, out_o,
    pgm, dd, xr, mom_v, nm_v,
    hid_v, w_v, wt_v, og_v, po, lrecv, lay_v, part, brecv, fin, xs, xrv, hg_v,
    load_sem, give_sem, rs_sem, ag_sem, pass_sem, g_sem, l_sem, b_sem, e_sem, h_sem, z_sem,
):
    n_x, n_z, n_y = n_rep // 2, n_dp // 2, n_tp
    rep, dp, y = lax.axis_index("rep"), lax.axis_index("dp"), lax.axis_index("tp")
    x, core = rep // 2, rep % 2
    z, low = dp // 2, dp % 2
    units, width = w.shape
    shift = n_z // 2 - 1
    slot_me = lax.rem(y + (-shift) % n_z + n_z - z, n_z)
    partner = {"rep": 2 * x + 1 - core}
    pair = {"dp": 2 * z + 1 - low}
    order_x = sorted(range(n_x), key=lambda k: -min(k, n_x - k))
    barrier = pltpu.get_barrier_semaphore()

    def at_x(k):
        return lax.rem(x + k % n_x, n_x)

    def to_x(s):
        return {"rep": 2 * at_x(s) + core}

    def to_z(s):
        return {"dp": 2 * lax.rem(z + s % n_z, n_z) + low}

    def to_y(o):
        return {"tp": lax.rem(y + o % n_y, n_y)}

    def remote(src, dst, sems, i, where):
        return pltpu.make_async_remote_copy(
            src_ref=src, dst_ref=dst, send_sem=sems.at[0, i], recv_sem=sems.at[1, i],
            device_id=where, device_id_type=MESH,
        )

    def arrived(ref, sems, i):
        remote(ref, ref, sems, i, partner).wait_recv()

    def span(total, pieces, c):
        return pl.ds(c * (total // pieces), total // pieces)

    def sign_at(s):
        return 0 if s > 0 else 1

    def greet(peers):
        for where in peers:
            pl.semaphore_signal(barrier, inc=1, device_id=where, device_id_type=MESH)

    MOM, OG, HID, NM, LAY = range(n_x, n_x + 5)

    def x_program():
        sent, loads = [], {}

        def go(copy):
            copy.start()
            sent.append(copy)
            return copy

        def load(name, src, dst):
            loads[name] = pltpu.make_async_copy(src, dst, load_sem.at[len(loads)])
            loads[name].start()

        for k in order_x:
            load(k, pg.at[at_x(k)], pgm.at[k])
        load("mom", mom, mom_v.at[0])
        peers = [partner] + [to_x(s) for s in sorted({1 % n_x, -1 % n_x} - {0})]
        greet(peers)
        pl.semaphore_wait(barrier, len(peers))
        go(remote(og, og_v.at[0, slot_me], give_sem, OG, partner))
        go(remote(hid, hid_v.at[0], give_sem, HID, partner))

        index = {key: i for i, key in enumerate(ring_items(n_x, PIECES_X))}
        rs, ag, ready = {}, {}, set()

        def have(k):
            if k not in ready:
                ready.add(k)
                arrived(dd.at[k], give_sem, k)
                loads[k].wait()

        def rs_send(s, h, d, c):
            k = (s * d) % n_x
            cols = span(width, PIECES_X, c)
            total = pgm[k, h, :, cols].astype(F32) + dd[k, h, :, cols].astype(F32)
            if d < arm(n_x, s, h):
                rs[s, h, d + 1, c].wait_recv()
                total = total + xr[sign_at(s), h, d, :, cols].astype(F32)
            dd[k, h, :, cols] = total.astype(BF16)
            target = xr.at[sign_at(s), h, d - 1, :, cols]
            rs[s, h, d, c] = go(remote(dd.at[k, h, :, cols], target, rs_sem, index[s, h, d, c], to_x(s)))

        def hand_out(k, h, c):
            piece = out_o.at[at_x(k), h, :, span(width, PIECES_X, c)]
            go(remote(piece, piece, pass_sem, (k * 2 + h) * PIECES_X + c, partner))

        def ag_send(s, h, d, c):
            piece = out_o.at[at_x(-s * (d - 1)), h, :, span(width, PIECES_X, c)]
            ag[s, h, d, c] = go(remote(piece, piece, ag_sem, index[s, h, d, c], to_x(s)))

        def ag_take(s, h, d, c):
            ag[s, h, d, c].wait_recv()
            if d < arm(n_x, s, h):
                ag_send(s, h, d + 1, c)
            hand_out((-s * d) % n_x, h, c)

        def rs_end(c):
            have(0)
            cols = span(width, PIECES_X, c)
            for h in (0, 1):
                total = pgm[0, h, :, cols].astype(F32) + dd[0, h, :, cols].astype(F32)
                for s in (1, -1):
                    if arm(n_x, s, h) >= 1:
                        rs[s, h, 1, c].wait_recv()
                        total = total + xr[sign_at(s), h, 0, :, cols].astype(F32)
                average = total * (1.0 / n_rep)
                new = momentum_rate * mom_v[h, :, cols] + average
                if h == 0:
                    nm_o[:, cols] = new
                else:
                    nm_v[:, cols] = new
                out_o[x, h, :, cols] = (outer_rate * (average + momentum_rate * new)).astype(BF16)
            for far_first in (True, False):
                for s in (1, -1):
                    for h in (0, 1):
                        if arm(n_x, s, h) >= 1 and ((s > 0) == (h == 0)) == far_first:
                            ag_send(s, h, 1, c)
            for h in (0, 1):
                hand_out(0, h, c)

        starts = sorted(
            (c, -arm(n_x, s, h), s, h)
            for c in range(PIECES_X)
            for s in (1, -1)
            for h in (0, 1)
            if arm(n_x, s, h) >= 1
        )
        for c, d, s, h in starts:
            have((s * -d) % n_x)
            rs_send(s, h, -d, c)
        for c in range(PIECES_X):
            for d in range(n_x // 2 - 1, 0, -1):
                for s in (1, -1):
                    for h in (0, 1):
                        if d < arm(n_x, s, h):
                            rs_send(s, h, d, c)
        loads["mom"].wait()
        arrived(mom_v.at[1], give_sem, MOM)
        for c in range(PIECES_X):
            rs_end(c)
        go(remote(nm_v, nm_o, give_sem, NM, partner))
        for d in range(1, n_x // 2 + 1):
            for c in range(PIECES_X):
                for s in (1, -1):
                    for h in (0, 1):
                        if d <= arm(n_x, s, h):
                            ag_take(s, h, d, c)
        arrived(lay_o, give_sem, LAY)
        for c in range(PIECES_Z):
            arrived(hg_o.at[:, span(units, PIECES_Z, c)], h_sem, c)
        for copy in sent:
            copy.wait_send()

    def z_program():
        sent, loads = [], {}

        def go(copy):
            copy.start()
            sent.append(copy)
            return copy

        def load(name, src, dst):
            loads[name] = pltpu.make_async_copy(src, dst, load_sem.at[len(loads)])
            loads[name].start()

        load("og", og, og_v.at[1, slot_me])
        load("w", w, w_v)
        load("hid", hid, hid_v.at[1])

        peers = [partner, pair] + [to_y(o) for o in range(1, n_y)]
        greet(peers)
        lower_than = {1: z < n_z - 1, -1: z == 0}
        higher_than = {1: z == n_z - 1, -1: z > 0}
        if n_z > 1:
            for s in (1, -1):

                @pl.when(lower_than[s])
                def _():
                    greet([to_z(s)])

            pl.semaphore_wait(barrier, len(peers) + (z + n_z - 1) // n_z + (z + 1) // n_z)
            for s in (1, -1):

                @pl.when(higher_than[s])
                def _():
                    pl.semaphore_signal(z_sem.at[sign_at(-s)], inc=1, device_id=to_z(s), device_id_type=MESH)

        else:
            pl.semaphore_wait(barrier, len(peers))

        near, far = gather_plan(n_y)
        g_index = {(o, r): 2 * i + r for i, (o, _, _) in enumerate(near + far) for r in (0, 1)}
        gathers, relayed = {}, set()
        half_rows = og.shape[0] // 2

        def gather(o, relay, rows, r):
            if relay and (relay, r) not in relayed:
                relayed.add((relay, r))
                gathers[relay, r].wait_recv()
            ref = og_v.at[r, lax.rem(slot_me + (-relay) % n_z, n_z)]
            if rows < 2:
                ref = ref.at[pl.ds(rows * half_rows, half_rows)]
            gathers[o, r] = go(remote(ref, ref, g_sem, g_index[o, r], to_y(o - relay)))

        loads["og"].wait()
        for item in near:
            gather(*item, 1)
        for k in order_x:
            go(remote(pg.at[at_x(k)], dd.at[k], give_sem, k, partner))
        go(remote(mom, mom_v.at[1], give_sem, MOM, partner))
        arrived(og_v.at[0, slot_me], give_sem, OG)
        for item in near:
            gather(*item, 0)

        loads["w"].wait()
        f_tile = min(256, units)

        @pl.loop(0, units // f_tile)
        def _(j):
            cols = pl.ds(pl.multiple_of(j * f_tile, f_tile), f_tile)
            wt_v[:, cols] = w_v[cols, :].T

        for r in (1, 0):
            for item in far:
                gather(*item, r)

        loads["hid"].wait()
        arrived(hid_v.at[0], give_sem, HID)
        tile = min(256, width)

        @pl.loop(0, width // tile)
        def _(j):
            cols = pl.ds(pl.multiple_of(j * tile, tile), tile)
            for r in (0, 1):
                block = jnp.dot(hid_v[r], w_v[:, cols], preferred_element_type=F32)
                po[:, r, :, cols] = block.astype(BF16).reshape(n_y, -1, tile)

        for key in gathers:
            if key not in relayed:
                gathers[key].wait_recv()

        exchange = {}
        for o in range(1, n_y):
            exchange[o] = go(remote(po.at[lax.rem(y + o, n_y)], lrecv.at[o - 1], l_sem, o - 1, to_y(o)))

        def back(a, b):
            @pl.loop(0, units // f_tile)
            def _(j):
                cols = pl.ds(pl.multiple_of(j * f_tile, f_tile), f_tile)
                rows = og_v[:, pl.ds(a, b - a)].reshape(-1, width)
                block = jnp.dot(rows, wt_v[:, cols], preferred_element_type=F32).astype(BF16)
                block = block.reshape(2, b - a, 2, -1, f_tile)
                for r in (0, 1):
                    part[pl.ds(a, b - a), :, r, :, cols] = block[r]

        z_index = {key: i for i, key in enumerate(ring_items(n_z, PIECES_Z))}
        zs = {}

        def z_slot(k):
            return (k - shift) % n_z

        def z_send(s, h, d, c):
            k = z_slot(s * d)
            cols = span(units, PIECES_Z, c)
            if d < arm(n_z, s, h):
                zs[s, h, d + 1, c].wait_recv()
                total = part[k, h, :, :, cols].astype(F32) + brecv[sign_at(s), h, d, :, :, cols].astype(F32)
                part[k, h, :, :, cols] = total.astype(BF16)
            target = brecv.at[sign_at(s), h, d - 1, :, :, cols]
            zs[s, h, d, c] = go(remote(part.at[k, h, :, :, cols], target, b_sem, z_index[s, h, d, c], to_z(s)))

        def z_wave(step, long_arm):
            for c in range(PIECES_Z):
                for s in (1, -1):
                    h = 0 if (s > 0) == long_arm else 1
                    d = arm(n_z, s, h) - step
                    if d >= 1:
                        z_send(s, h, d, c)

        cut = min(3, n_z)
        back(0, cut)
        if n_z > 1:
            for s in (1, -1):

                @pl.when(lower_than[s])
                def _():
                    pl.semaphore_wait(z_sem.at[sign_at(s)], 1)

        z_wave(0, True)
        z_wave(0, False)
        if cut < n_z:
            back(cut, n_z)
        for step in range(1, n_z // 2):
            z_wave(step, True)
            z_wave(step, False)

        ends = {}
        for c in range(PIECES_Z):
            cols = span(units, PIECES_Z, c)
            for h in (0, 1):
                total = part[z_slot(0), h, :, :, cols].astype(F32)
                for s in (1, -1):
                    if arm(n_z, s, h) >= 1:
                        zs[s, h, 1, c].wait_recv()
                        total = total + brecv[sign_at(s), h, 0, :, :, cols].astype(F32)
                fin[h, :, :, cols] = total
            xs[:, :, cols] = fin[1 - low, :, :, cols].astype(BF16)
            ends[c] = go(remote(xs.at[:, :, cols], xrv.at[:, :, cols], e_sem, c, pair))

        total = po[y].astype(F32)
        for o in range(1, n_y):
            exchange[o].wait_recv()
            total = total + lrecv[o - 1].astype(F32)
        lay_v[...] = total[0].astype(BF16)
        lay_o[...] = total[1].astype(BF16)
        go(remote(lay_v, lay_o, give_sem, LAY, partner))

        for c in range(PIECES_Z):
            cols = span(units, PIECES_Z, c)
            ends[c].wait_recv()
            total = fin[low, :, :, cols] + xrv[:, :, cols].astype(F32)
            hg_v[:, cols] = total[0].astype(BF16)
            hg_o[:, cols] = total[1].astype(BF16)
            go(remote(hg_v.at[:, cols], hg_o.at[:, cols], h_sem, c, partner))

        for k in range(n_x):
            for h in (0, 1):
                for c in range(PIECES_X):
                    piece = out_o.at[at_x(k), h, :, span(width, PIECES_X, c)]
                    arrived(piece, pass_sem, (k * 2 + h) * PIECES_X + c)
        arrived(nm_o, give_sem, NM)
        for copy in sent:
            copy.wait_send()

    pl.when(core == 0)(x_program)
    pl.when(core == 1)(z_program)


def store(*refs):
    copies = [pltpu.make_async_copy(refs[i], refs[4 + i], refs[8].at[i]) for i in range(4)]
    for copy in copies:
        copy.start()
    for copy in copies:
        copy.wait()


def per_device(sizes, hidden, down_weight, out_grad, pseudo_grad, momentum):
    n_rep, n_dp, n_tp = sizes
    n_x, n_z = n_rep // 2, n_dp // 2
    tokens, units = hidden.shape[1:]
    width = down_weight.shape[1]
    rows = out_grad.shape[1]
    share = momentum.shape[0]
    owned = tokens // n_dp
    far_x, far_z = max(n_x // 2, 1), max(n_z // 2, 1)
    x_copies = max(len(ring_items(n_x, PIECES_X)), 1)
    z_copies = max(len(ring_items(n_z, PIECES_Z)), 1)
    near, far = gather_plan(n_tp)
    any_ref = pl.BlockSpec(memory_space=pl.ANY)
    vmem = pl.BlockSpec(memory_space=pltpu.VMEM)
    sem = pltpu.SemaphoreType.DMA
    results = pl.pallas_call(
        functools.partial(kernel, n_rep, n_dp, n_tp),
        out_shape=(
            pltpu.VMEM((rows, width), BF16),
            pltpu.VMEM((owned, units), BF16),
            pltpu.VMEM((share, width), F32),
            pltpu.VMEM((n_x, 2, share, width), BF16),
        ),
        in_specs=[any_ref] * 5,
        out_specs=(vmem,) * 4,
        scratch_shapes=[
            pltpu.VMEM((n_x, 2, share, width), BF16),
            pltpu.VMEM((n_x, 2, share, width), BF16),
            pltpu.VMEM((2, 2, far_x, share, width), BF16),
            pltpu.VMEM((2, share, width), F32),
            pltpu.VMEM((share, width), F32),
            pltpu.VMEM((2, tokens, units), BF16),
            pltpu.VMEM((units, width), BF16),
            pltpu.VMEM((width, units), BF16),
            pltpu.VMEM((2, n_tp, rows, width), BF16),
            pltpu.VMEM((n_tp, 2, rows, width), BF16),
            pltpu.VMEM((max(n_tp - 1, 1), 2, rows, width), BF16),
            pltpu.VMEM((rows, width), BF16),
            pltpu.VMEM((n_z, 2, 2, owned, units), BF16),
            pltpu.VMEM((2, 2, far_z, 2, owned, units), BF16),
            pltpu.VMEM((2, 2, owned, units), F32),
            pltpu.VMEM((2, owned, units), BF16),
            pltpu.VMEM((2, owned, units), BF16),
            pltpu.VMEM((owned, units), BF16),
            sem((max(n_x + 1, 3),)),
            sem((2, n_x + 5)),
            sem((2, x_copies)),
            sem((2, x_copies)),
            sem((2, 2 * n_x * PIECES_X)),
            sem((2, max(2 * len(near + far), 1))),
            sem((2, max(n_tp - 1, 1))),
            sem((2, z_copies)),
            sem((2, PIECES_Z)),
            sem((2, PIECES_Z)),
            pltpu.SemaphoreType.REGULAR((2,)),
        ],
        compiler_params=pltpu.CompilerParams(collective_id=0, has_side_effects=True),
        name="step",
    )(
        hidden[0],
        down_weight,
        out_grad[0],
        pseudo_grad.reshape(n_x, 2, share, width),
        momentum,
    )
    lay, hg, nm, out = pl.pallas_call(
        store,
        out_shape=tuple(jax.ShapeDtypeStruct(r.shape, r.dtype) for r in results),
        in_specs=[vmem] * 4,
        out_specs=(any_ref,) * 4,
        scratch_shapes=[sem((4,))],
        compiler_params=pltpu.CompilerParams(vmem_limit_bytes=1 << 20),
        name="store",
    )(*results)
    return lay[None], hg[None], nm, out.reshape(down_weight.shape)


def solution(mesh):
    sizes = tuple(mesh.shape[axis] for axis in ("rep", "dp", "tp"))
    return jax.shard_map(
        functools.partial(per_device, sizes),
        mesh=mesh,
        in_specs=(
            P("rep", None, "tp"),
            P("tp", "dp"),
            P("rep", "tp", "dp"),
            P("rep", "tp", "dp"),
            P(("tp", "rep"), "dp"),
        ),
        out_specs=(
            P("rep", "tp", "dp"),
            P("rep", "dp", "tp"),
            P(("tp", "rep"), "dp"),
            P("tp", "dp"),
        ),
        check_vma=False,
    )
```

```python
import functools

import jax
import jax.numpy as jnp
from jax import lax
from jax.experimental import pallas as pl
from jax.experimental.pallas import tpu as pltpu
from jax.sharding import PartitionSpec as P

outer_rate = 0.7
momentum_rate = 0.9
MESH = pl.DeviceIdType.MESH
F32, BF16 = jnp.float32, jnp.bfloat16
PIECES_X = 2
PIECES_Z = 2


def arm(n, sign, half):
    return n // 2 - (0 if (sign > 0) == (half == 0) else 1)


def ring_items(n, pieces):
    return [
        (s, h, d, c)
        for s in (1, -1)
        for h in (0, 1)
        for d in range(1, arm(n, s, h) + 1)
        for c in range(pieces)
    ]


def gather_plan(n):
    if n == 8:
        near = [(2, 0, 2), (-2, 0, 2), (1, 0, 2), (-1, 0, 2)]
        far = [(4, 2, 0), (-4, -2, 1), (3, 2, 2), (-3, -2, 2)]
        return near, far
    return [(o, 0, 2) for o in range(1, n)], []


def kernel(
    n_rep, n_dp, n_tp,
    hid, w, og, pg, mom,
    lay_o, hg_o, nm_o, out_o,
    pgm, dd, xr, mom_v, nm_v,
    hid_v, w_v, wt_v, og_v, po, lrecv, lay_v, part, brecv, fin, xs, xrv, hg_v,
    load_sem, give_sem, rs_sem, ag_sem, pass_sem, g_sem, l_sem, b_sem, e_sem, h_sem, z_sem,
):
    n_x, n_z, n_y = n_rep // 2, n_dp // 2, n_tp
    rep, dp, y = lax.axis_index("rep"), lax.axis_index("dp"), lax.axis_index("tp")
    x, core = rep // 2, rep % 2
    z, low = dp // 2, dp % 2
    units, width = w.shape
    shift = n_z // 2 - 1
    slot_me = lax.rem(y + (-shift) % n_z + n_z - z, n_z)
    partner = {"rep": 2 * x + 1 - core}
    pair = {"dp": 2 * z + 1 - low}
    order_x = sorted(range(n_x), key=lambda k: -min(k, n_x - k))
    barrier = pltpu.get_barrier_semaphore()

    def at_x(k):
        return lax.rem(x + k % n_x, n_x)

    def to_x(s):
        return {"rep": 2 * at_x(s) + core}

    def to_z(s):
        return {"dp": 2 * lax.rem(z + s % n_z, n_z) + low}

    def to_y(o):
        return {"tp": lax.rem(y + o % n_y, n_y)}

    def remote(src, dst, sems, i, where):
        return pltpu.make_async_remote_copy(
            src_ref=src, dst_ref=dst, send_sem=sems.at[0, i], recv_sem=sems.at[1, i],
            device_id=where, device_id_type=MESH,
        )

    def arrived(ref, sems, i):
        remote(ref, ref, sems, i, partner).wait_recv()

    def span(total, pieces, c):
        return pl.ds(c * (total // pieces), total // pieces)

    def sign_at(s):
        return 0 if s > 0 else 1

    def greet(peers):
        for where in peers:
            pl.semaphore_signal(barrier, inc=1, device_id=where, device_id_type=MESH)

    MOM, OG, HID, NM, LAY = range(n_x * PIECES_X, n_x * PIECES_X + 5)

    def x_program():
        sent, loads = [], {}

        def go(copy):
            copy.start()
            sent.append(copy)
            return copy

        def load(name, src, dst):
            loads[name] = pltpu.make_async_copy(src, dst, load_sem.at[len(loads)])
            loads[name].start()

        for k in order_x:
            load(k, pg.at[at_x(k)], pgm.at[k])
        load("mom", mom, mom_v.at[0])
        peers = [partner] + [to_x(s) for s in sorted({1 % n_x, -1 % n_x} - {0})]
        greet(peers)
        pl.semaphore_wait(barrier, len(peers))
        go(remote(og, og_v.at[0, slot_me], give_sem, OG, partner))
        go(remote(hid, hid_v.at[0], give_sem, HID, partner))

        index = {key: i for i, key in enumerate(ring_items(n_x, PIECES_X))}
        rs, ag, ready = {}, {}, set()

        def have(k, c):
            if (k, c) not in ready:
                ready.add((k, c))
                arrived(dd.at[k, :, :, span(width, PIECES_X, c)], give_sem, k * PIECES_X + c)
            if k not in ready:
                ready.add(k)
                loads[k].wait()

        def rs_send(s, h, d, c):
            k = (s * d) % n_x
            cols = span(width, PIECES_X, c)
            total = pgm[k, h, :, cols].astype(F32) + dd[k, h, :, cols].astype(F32)
            if d < arm(n_x, s, h):
                rs[s, h, d + 1, c].wait_recv()
                total = total + xr[sign_at(s), h, d, :, cols].astype(F32)
            dd[k, h, :, cols] = total.astype(BF16)
            target = xr.at[sign_at(s), h, d - 1, :, cols]
            rs[s, h, d, c] = go(remote(dd.at[k, h, :, cols], target, rs_sem, index[s, h, d, c], to_x(s)))

        def hand_out(k, h, c):
            piece = out_o.at[at_x(k), h, :, span(width, PIECES_X, c)]
            go(remote(piece, piece, pass_sem, (k * 2 + h) * PIECES_X + c, partner))

        def ag_send(s, h, d, c):
            piece = out_o.at[at_x(-s * (d - 1)), h, :, span(width, PIECES_X, c)]
            ag[s, h, d, c] = go(remote(piece, piece, ag_sem, index[s, h, d, c], to_x(s)))

        def ag_take(s, h, d, c):
            ag[s, h, d, c].wait_recv()
            if d < arm(n_x, s, h):
                ag_send(s, h, d + 1, c)
            hand_out((-s * d) % n_x, h, c)

        def rs_end(c):
            have(0, c)
            cols = span(width, PIECES_X, c)
            for h in (0, 1):
                total = pgm[0, h, :, cols].astype(F32) + dd[0, h, :, cols].astype(F32)
                for s in (1, -1):
                    if arm(n_x, s, h) >= 1:
                        rs[s, h, 1, c].wait_recv()
                        total = total + xr[sign_at(s), h, 0, :, cols].astype(F32)
                average = total * (1.0 / n_rep)
                new = momentum_rate * mom_v[h, :, cols] + average
                if h == 0:
                    nm_o[:, cols] = new
                else:
                    nm_v[:, cols] = new
                out_o[x, h, :, cols] = (outer_rate * (average + momentum_rate * new)).astype(BF16)
            for far_first in (True, False):
                for s in (1, -1):
                    for h in (0, 1):
                        if arm(n_x, s, h) >= 1 and ((s > 0) == (h == 0)) == far_first:
                            ag_send(s, h, 1, c)
            for h in (0, 1):
                hand_out(0, h, c)

        starts = sorted(
            (c, -arm(n_x, s, h), s, h)
            for c in range(PIECES_X)
            for s in (1, -1)
            for h in (0, 1)
            if arm(n_x, s, h) >= 1
        )
        for c, d, s, h in starts:
            have((s * -d) % n_x, c)
            rs_send(s, h, -d, c)
        for c in range(PIECES_X):
            for d in range(n_x // 2 - 1, 0, -1):
                for s in (1, -1):
                    for h in (0, 1):
                        if d < arm(n_x, s, h):
                            rs_send(s, h, d, c)
        loads["mom"].wait()
        arrived(mom_v.at[1], give_sem, MOM)
        for c in range(PIECES_X):
            rs_end(c)
        go(remote(nm_v, nm_o, give_sem, NM, partner))
        for d in range(1, n_x // 2 + 1):
            for c in range(PIECES_X):
                for s in (1, -1):
                    for h in (0, 1):
                        if d <= arm(n_x, s, h):
                            ag_take(s, h, d, c)
        arrived(lay_o, give_sem, LAY)
        for c in range(PIECES_Z):
            arrived(hg_o.at[:, span(units, PIECES_Z, c)], h_sem, c)
        for copy in sent:
            copy.wait_send()

    def z_program():
        sent, loads = [], {}

        def go(copy):
            copy.start()
            sent.append(copy)
            return copy

        def load(name, src, dst):
            loads[name] = pltpu.make_async_copy(src, dst, load_sem.at[len(loads)])
            loads[name].start()

        load("og", og, og_v.at[1, slot_me])
        load("w", w, w_v)
        load("hid", hid, hid_v.at[1])

        peers = [partner, pair] + [to_y(o) for o in range(1, n_y)]
        greet(peers)
        lower_than = {1: z < n_z - 1, -1: z == 0}
        higher_than = {1: z == n_z - 1, -1: z > 0}
        if n_z > 1:
            for s in (1, -1):

                @pl.when(lower_than[s])
                def _():
                    greet([to_z(s)])

            pl.semaphore_wait(barrier, len(peers) + (z + n_z - 1) // n_z + (z + 1) // n_z)
            for s in (1, -1):

                @pl.when(higher_than[s])
                def _():
                    pl.semaphore_signal(z_sem.at[sign_at(-s)], inc=1, device_id=to_z(s), device_id_type=MESH)

        else:
            pl.semaphore_wait(barrier, len(peers))

        near, far = gather_plan(n_y)
        g_index = {(o, r): 2 * i + r for i, (o, _, _) in enumerate(near + far) for r in (0, 1)}
        gathers, relayed = {}, set()
        half_rows = og.shape[0] // 2

        def gather(o, relay, rows, r):
            if relay and (relay, r) not in relayed:
                relayed.add((relay, r))
                gathers[relay, r].wait_recv()
            ref = og_v.at[r, lax.rem(slot_me + (-relay) % n_z, n_z)]
            if rows < 2:
                ref = ref.at[pl.ds(rows * half_rows, half_rows)]
            gathers[o, r] = go(remote(ref, ref, g_sem, g_index[o, r], to_y(o - relay)))

        tile, f_tile = min(512, width), min(256, units)

        def forward(r):
            @pl.loop(0, width // tile)
            def _(j):
                cols = pl.ds(pl.multiple_of(j * tile, tile), tile)
                block = jnp.dot(hid_v[r], w_v[:, cols], preferred_element_type=F32)
                po[:, r, :, cols] = block.astype(BF16).reshape(n_y, -1, tile)

        def gathered(r):
            for key in gathers:
                if key[1] == r and key not in relayed:
                    gathers[key].wait_recv()

        loads["og"].wait()
        for item in near:
            gather(*item, 1)
        for c in range(PIECES_X):
            for k in order_x:
                cols = span(width, PIECES_X, c)
                target = dd.at[k, :, :, cols]
                go(remote(pg.at[at_x(k), :, :, cols], target, give_sem, k * PIECES_X + c, partner))
        go(remote(mom, mom_v.at[1], give_sem, MOM, partner))
        loads["w"].wait()
        loads["hid"].wait()
        forward(1)
        for item in far:
            gather(*item, 1)
        arrived(og_v.at[0, slot_me], give_sem, OG)
        for item in near:
            gather(*item, 0)

        @pl.loop(0, units // f_tile)
        def _(j):
            cols = pl.ds(pl.multiple_of(j * f_tile, f_tile), f_tile)
            wt_v[:, cols] = w_v[cols, :].T

        def back(a, b, r):
            wide = units // 2

            @pl.loop(0, 2)
            def _(j):
                cols = pl.ds(pl.multiple_of(j * wide, wide), wide)
                rows = og_v[r, pl.ds(a, b - a)].reshape(-1, width)
                block = jnp.dot(rows, wt_v[:, cols], preferred_element_type=F32).astype(BF16)
                part[pl.ds(a, b - a), :, r, :, cols] = block.reshape(b - a, 2, -1, wide)

        z_index = {key: i for i, key in enumerate(ring_items(n_z, 2 * PIECES_Z))}
        zs = {}

        def z_slot(k):
            return (k - shift) % n_z

        def z_send(s, h, d, r, c):
            k = z_slot(s * d)
            cols = span(units, PIECES_Z, c)
            i = r * PIECES_Z + c
            if d < arm(n_z, s, h):
                zs[s, h, d + 1, i].wait_recv()
                total = part[k, h, r, :, cols].astype(F32) + brecv[sign_at(s), h, d, r, :, cols].astype(F32)
                part[k, h, r, :, cols] = total.astype(BF16)
            target = brecv.at[sign_at(s), h, d - 1, r, :, cols]
            zs[s, h, d, i] = go(remote(part.at[k, h, r, :, cols], target, b_sem, z_index[s, h, d, i], to_z(s)))

        def z_wave(step, r):
            for long_arm in (True, False):
                for c in range(PIECES_Z):
                    for s in (1, -1):
                        h = 0 if (s > 0) == long_arm else 1
                        d = arm(n_z, s, h) - step
                        if d >= 1:
                            z_send(s, h, d, r, c)

        ends = {}

        def z_end(r):
            for c in range(PIECES_Z):
                i = r * PIECES_Z + c
                cols = span(units, PIECES_Z, c)
                for h in (0, 1):
                    total = part[z_slot(0), h, r, :, cols].astype(F32)
                    for s in (1, -1):
                        if arm(n_z, s, h) >= 1:
                            zs[s, h, 1, i].wait_recv()
                            total = total + brecv[sign_at(s), h, 0, r, :, cols].astype(F32)
                    fin[h, r, :, cols] = total
                xs[r, :, cols] = fin[1 - low, r, :, cols].astype(BF16)
                ends[i] = go(remote(xs.at[r, :, cols], xrv.at[r, :, cols], e_sem, i, pair))

        def grad_out(r):
            for c in range(PIECES_Z):
                i = r * PIECES_Z + c
                cols = span(units, PIECES_Z, c)
                ends[i].wait_recv()
                total = (fin[low, r, :, cols] + xrv[r, :, cols].astype(F32)).astype(BF16)
                if r == 1:
                    hg_o[:, cols] = total
                else:
                    hg_v[:, cols] = total
                    go(remote(hg_v.at[:, cols], hg_o.at[:, cols], h_sem, c, partner))

        cut = min(3, n_z)
        last = n_z // 2 - 1
        gathered(1)
        back(0, cut, 1)
        if n_z > 1:
            for s in (1, -1):

                @pl.when(lower_than[s])
                def _():
                    pl.semaphore_wait(z_sem.at[sign_at(s)], 1)

        z_wave(0, 1)
        for item in far:
            gather(*item, 0)
        if cut < n_z:
            back(cut, n_z, 1)
        arrived(hid_v.at[0], give_sem, HID)
        if last >= 1:
            z_wave(1, 1)
        gathered(0)
        back(0, cut, 0)
        z_wave(0, 0)
        forward(0)
        exchange = {}
        for o in range(1, n_y):
            exchange[o] = go(remote(po.at[lax.rem(y + o, n_y)], lrecv.at[o - 1], l_sem, o - 1, to_y(o)))
        if cut < n_z:
            back(cut, n_z, 0)
        for step in range(2, last + 1):
            z_wave(step, 1)
            z_wave(step - 1, 0)
        z_end(1)
        if last >= 1:
            z_wave(last, 0)
        z_end(0)
        grad_out(1)

        total = po[y].astype(F32)
        for o in range(1, n_y):
            exchange[o].wait_recv()
            total = total + lrecv[o - 1].astype(F32)
        lay_v[...] = total[0].astype(BF16)
        lay_o[...] = total[1].astype(BF16)
        go(remote(lay_v, lay_o, give_sem, LAY, partner))
        grad_out(0)

        for k in range(n_x):
            for h in (0, 1):
                for c in range(PIECES_X):
                    piece = out_o.at[at_x(k), h, :, span(width, PIECES_X, c)]
                    arrived(piece, pass_sem, (k * 2 + h) * PIECES_X + c)
        arrived(nm_o, give_sem, NM)
        for copy in sent:
            copy.wait_send()

    pl.when(core == 0)(x_program)
    pl.when(core == 1)(z_program)


def store(*refs):
    copies = [pltpu.make_async_copy(refs[i], refs[4 + i], refs[8].at[i]) for i in range(4)]
    for copy in copies:
        copy.start()
    for copy in copies:
        copy.wait()


def per_device(sizes, hidden, down_weight, out_grad, pseudo_grad, momentum):
    n_rep, n_dp, n_tp = sizes
    n_x, n_z = n_rep // 2, n_dp // 2
    tokens, units = hidden.shape[1:]
    width = down_weight.shape[1]
    rows = out_grad.shape[1]
    share = momentum.shape[0]
    owned = tokens // n_dp
    far_x, far_z = max(n_x // 2, 1), max(n_z // 2, 1)
    x_copies = max(len(ring_items(n_x, PIECES_X)), 1)
    z_copies = max(len(ring_items(n_z, 2 * PIECES_Z)), 1)
    near, far = gather_plan(n_tp)
    any_ref = pl.BlockSpec(memory_space=pl.ANY)
    vmem = pl.BlockSpec(memory_space=pltpu.VMEM)
    sem = pltpu.SemaphoreType.DMA
    results = pl.pallas_call(
        functools.partial(kernel, n_rep, n_dp, n_tp),
        out_shape=(
            pltpu.VMEM((rows, width), BF16),
            pltpu.VMEM((owned, units), BF16),
            pltpu.VMEM((share, width), F32),
            pltpu.VMEM((n_x, 2, share, width), BF16),
        ),
        in_specs=[any_ref] * 5,
        out_specs=(vmem,) * 4,
        scratch_shapes=[
            pltpu.VMEM((n_x, 2, share, width), BF16),
            pltpu.VMEM((n_x, 2, share, width), BF16),
            pltpu.VMEM((2, 2, far_x, share, width), BF16),
            pltpu.VMEM((2, share, width), F32),
            pltpu.VMEM((share, width), F32),
            pltpu.VMEM((2, tokens, units), BF16),
            pltpu.VMEM((units, width), BF16),
            pltpu.VMEM((width, units), BF16),
            pltpu.VMEM((2, n_tp, rows, width), BF16),
            pltpu.VMEM((n_tp, 2, rows, width), BF16),
            pltpu.VMEM((max(n_tp - 1, 1), 2, rows, width), BF16),
            pltpu.VMEM((rows, width), BF16),
            pltpu.VMEM((n_z, 2, 2, owned, units), BF16),
            pltpu.VMEM((2, 2, far_z, 2, owned, units), BF16),
            pltpu.VMEM((2, 2, owned, units), F32),
            pltpu.VMEM((2, owned, units), BF16),
            pltpu.VMEM((2, owned, units), BF16),
            pltpu.VMEM((owned, units), BF16),
            sem((max(n_x + 1, 3),)),
            sem((2, n_x * PIECES_X + 5)),
            sem((2, x_copies)),
            sem((2, x_copies)),
            sem((2, 2 * n_x * PIECES_X)),
            sem((2, max(2 * len(near + far), 1))),
            sem((2, max(n_tp - 1, 1))),
            sem((2, z_copies)),
            sem((2, 2 * PIECES_Z)),
            sem((2, PIECES_Z)),
            pltpu.SemaphoreType.REGULAR((2,)),
        ],
        compiler_params=pltpu.CompilerParams(collective_id=0, has_side_effects=True),
        name="step",
    )(
        hidden[0],
        down_weight,
        out_grad[0],
        pseudo_grad.reshape(n_x, 2, share, width),
        momentum,
    )
    lay, hg, nm, out = pl.pallas_call(
        store,
        out_shape=tuple(jax.ShapeDtypeStruct(r.shape, r.dtype) for r in results),
        in_specs=[vmem] * 4,
        out_specs=(any_ref,) * 4,
        scratch_shapes=[sem((4,))],
        compiler_params=pltpu.CompilerParams(vmem_limit_bytes=1 << 20),
        name="store",
    )(*results)
    return lay[None], hg[None], nm, out.reshape(down_weight.shape)


def solution(mesh):
    sizes = tuple(mesh.shape[axis] for axis in ("rep", "dp", "tp"))
    return jax.shard_map(
        functools.partial(per_device, sizes),
        mesh=mesh,
        in_specs=(
            P("rep", None, "tp"),
            P("tp", "dp"),
            P("rep", "tp", "dp"),
            P("rep", "tp", "dp"),
            P(("tp", "rep"), "dp"),
        ),
        out_specs=(
            P("rep", "tp", "dp"),
            P("rep", "dp", "tp"),
            P(("tp", "rep"), "dp"),
            P("tp", "dp"),
        ),
        check_vma=False,
    )
```

```python
import functools

import jax
import jax.numpy as jnp
from jax import lax
from jax.experimental import pallas as pl
from jax.experimental.pallas import tpu as pltpu
from jax.sharding import PartitionSpec as P

outer_rate = 0.7
momentum_rate = 0.9
MESH = pl.DeviceIdType.MESH
F32, BF16 = jnp.float32, jnp.bfloat16
PIECES_X = 2
PIECES_Z = 2


def arm(n, sign, half):
    return n // 2 - (0 if (sign > 0) == (half == 0) else 1)


def ring_items(n, pieces):
    return [
        (s, h, d, c)
        for s in (1, -1)
        for h in (0, 1)
        for d in range(1, arm(n, s, h) + 1)
        for c in range(pieces)
    ]


def gather_plan(n):
    if n == 8:
        near = [(2, 0, 2), (-2, 0, 2), (1, 0, 2), (-1, 0, 2)]
        far = [(4, 2, 0), (-4, -2, 1), (3, 2, 2), (-3, -2, 2)]
        return near, far
    return [(o, 0, 2) for o in range(1, n)], []


def kernel(
    n_rep, n_dp, n_tp,
    hid, w, og, pg, mom,
    lay_o, hg_o, nm_o, out_o,
    pgm, dd, xr, mom_v, nm_v,
    hid_v, w_v, wt_v, og_v, po, lrecv, lay_v, part, brecv, fin, xs, xrv, hg_v,
    load_sem, give_sem, rs_sem, ag_sem, pass_sem, g_sem, l_sem, b_sem, e_sem, h_sem, z_sem,
):
    n_x, n_z, n_y = n_rep // 2, n_dp // 2, n_tp
    rep, dp, y = lax.axis_index("rep"), lax.axis_index("dp"), lax.axis_index("tp")
    x, core = rep // 2, rep % 2
    z, low = dp // 2, dp % 2
    units, width = w.shape
    shift = n_z // 2 - 1
    slot_me = lax.rem(y + (-shift) % n_z + n_z - z, n_z)
    partner = {"rep": 2 * x + 1 - core}
    pair = {"dp": 2 * z + 1 - low}
    order_x = sorted(range(n_x), key=lambda k: -min(k, n_x - k))
    barrier = pltpu.get_barrier_semaphore()

    def at_x(k):
        return lax.rem(x + k % n_x, n_x)

    def to_x(s):
        return {"rep": 2 * at_x(s) + core}

    def to_z(s):
        return {"dp": 2 * lax.rem(z + s % n_z, n_z) + low}

    def to_y(o):
        return {"tp": lax.rem(y + o % n_y, n_y)}

    def remote(src, dst, sems, i, where):
        return pltpu.make_async_remote_copy(
            src_ref=src, dst_ref=dst, send_sem=sems.at[0, i], recv_sem=sems.at[1, i],
            device_id=where, device_id_type=MESH,
        )

    def arrived(ref, sems, i):
        remote(ref, ref, sems, i, partner).wait_recv()

    def span(total, pieces, c):
        return pl.ds(c * (total // pieces), total // pieces)

    def sign_at(s):
        return 0 if s > 0 else 1

    def greet(peers):
        for where in peers:
            pl.semaphore_signal(barrier, inc=1, device_id=where, device_id_type=MESH)

    MOM, OG, HID, NM, LAY = range(n_x * PIECES_X, n_x * PIECES_X + 5)

    def x_program():
        sent, loads = [], {}

        def go(copy):
            copy.start()
            sent.append(copy)
            return copy

        def load(name, src, dst):
            loads[name] = pltpu.make_async_copy(src, dst, load_sem.at[len(loads)])
            loads[name].start()

        for k in order_x:
            load(k, pg.at[at_x(k)], pgm.at[k])
        load("mom", mom, mom_v.at[0])
        peers = [partner] + [to_x(s) for s in sorted({1 % n_x, -1 % n_x} - {0})]
        greet(peers)
        pl.semaphore_wait(barrier, len(peers))
        go(remote(og, og_v.at[0, slot_me], give_sem, OG, partner))
        go(remote(hid, hid_v.at[0], give_sem, HID, partner))

        index = {key: i for i, key in enumerate(ring_items(n_x, PIECES_X))}
        rs, ag, ready = {}, {}, set()

        def have(k, c):
            if (k, c) not in ready:
                ready.add((k, c))
                arrived(dd.at[k, :, :, span(width, PIECES_X, c)], give_sem, k * PIECES_X + c)
            if k not in ready:
                ready.add(k)
                loads[k].wait()

        def rs_send(s, h, d, c):
            k = (s * d) % n_x
            cols = span(width, PIECES_X, c)
            total = pgm[k, h, :, cols].astype(F32) + dd[k, h, :, cols].astype(F32)
            if d < arm(n_x, s, h):
                rs[s, h, d + 1, c].wait_recv()
                total = total + xr[sign_at(s), h, d, :, cols].astype(F32)
            dd[k, h, :, cols] = total.astype(BF16)
            target = xr.at[sign_at(s), h, d - 1, :, cols]
            rs[s, h, d, c] = go(remote(dd.at[k, h, :, cols], target, rs_sem, index[s, h, d, c], to_x(s)))

        def hand_out(k, h, c):
            piece = out_o.at[at_x(k), h, :, span(width, PIECES_X, c)]
            go(remote(piece, piece, pass_sem, (k * 2 + h) * PIECES_X + c, partner))

        def ag_send(s, h, d, c):
            piece = out_o.at[at_x(-s * (d - 1)), h, :, span(width, PIECES_X, c)]
            ag[s, h, d, c] = go(remote(piece, piece, ag_sem, index[s, h, d, c], to_x(s)))

        def ag_take(s, h, d, c):
            ag[s, h, d, c].wait_recv()
            if d < arm(n_x, s, h):
                ag_send(s, h, d + 1, c)
            hand_out((-s * d) % n_x, h, c)

        def rs_end(c):
            have(0, c)
            cols = span(width, PIECES_X, c)
            for h in (0, 1):
                total = pgm[0, h, :, cols].astype(F32) + dd[0, h, :, cols].astype(F32)
                for s in (1, -1):
                    if arm(n_x, s, h) >= 1:
                        rs[s, h, 1, c].wait_recv()
                        total = total + xr[sign_at(s), h, 0, :, cols].astype(F32)
                average = total * (1.0 / n_rep)
                new = momentum_rate * mom_v[h, :, cols] + average
                if h == 0:
                    nm_o[:, cols] = new
                else:
                    nm_v[:, cols] = new
                out_o[x, h, :, cols] = (outer_rate * (average + momentum_rate * new)).astype(BF16)
            for far_first in (True, False):
                for s in (1, -1):
                    for h in (0, 1):
                        if arm(n_x, s, h) >= 1 and ((s > 0) == (h == 0)) == far_first:
                            ag_send(s, h, 1, c)
            for h in (0, 1):
                hand_out(0, h, c)

        starts = sorted(
            (c, -arm(n_x, s, h), s, h)
            for c in range(PIECES_X)
            for s in (1, -1)
            for h in (0, 1)
            if arm(n_x, s, h) >= 1
        )
        for c, d, s, h in starts:
            have((s * -d) % n_x, c)
            rs_send(s, h, -d, c)
        for c in range(PIECES_X):
            for d in range(n_x // 2 - 1, 0, -1):
                for s in (1, -1):
                    for h in (0, 1):
                        if d < arm(n_x, s, h):
                            rs_send(s, h, d, c)
        loads["mom"].wait()
        arrived(mom_v.at[1], give_sem, MOM)
        for c in range(PIECES_X):
            rs_end(c)
        go(remote(nm_v, nm_o, give_sem, NM, partner))
        for d in range(1, n_x // 2 + 1):
            for c in range(PIECES_X):
                for far_first in (True, False):
                    for s in (1, -1):
                        h = 0 if (s > 0) == far_first else 1
                        if d <= arm(n_x, s, h):
                            ag_take(s, h, d, c)
        arrived(lay_o, give_sem, LAY)
        for c in range(PIECES_Z):
            arrived(hg_o.at[:, span(units, PIECES_Z, c)], h_sem, c)
        for copy in sent:
            copy.wait_send()

    def z_program():
        sent, loads = [], {}

        def go(copy):
            copy.start()
            sent.append(copy)
            return copy

        def load(name, src, dst):
            loads[name] = pltpu.make_async_copy(src, dst, load_sem.at[len(loads)])
            loads[name].start()

        load("og", og, og_v.at[1, slot_me])
        load("w", w, w_v)
        load("hid", hid, hid_v.at[1])

        peers = [partner, pair] + [to_y(o) for o in range(1, n_y)]
        greet(peers)
        lower_than = {1: z < n_z - 1, -1: z == 0}
        higher_than = {1: z == n_z - 1, -1: z > 0}
        if n_z > 1:
            for s in (1, -1):

                @pl.when(lower_than[s])
                def _():
                    greet([to_z(s)])

            pl.semaphore_wait(barrier, len(peers) + (z + n_z - 1) // n_z + (z + 1) // n_z)
            for s in (1, -1):

                @pl.when(higher_than[s])
                def _():
                    pl.semaphore_signal(z_sem.at[sign_at(-s)], inc=1, device_id=to_z(s), device_id_type=MESH)

        else:
            pl.semaphore_wait(barrier, len(peers))

        near, far = gather_plan(n_y)
        g_index = {(o, r): 2 * i + r for i, (o, _, _) in enumerate(near + far) for r in (0, 1)}
        gathers, relayed = {}, set()
        half_rows = og.shape[0] // 2

        def gather(o, relay, rows, r):
            if relay and (relay, r) not in relayed:
                relayed.add((relay, r))
                gathers[relay, r].wait_recv()
            ref = og_v.at[r, lax.rem(slot_me + (-relay) % n_z, n_z)]
            if rows < 2:
                ref = ref.at[pl.ds(rows * half_rows, half_rows)]
            gathers[o, r] = go(remote(ref, ref, g_sem, g_index[o, r], to_y(o - relay)))

        tile, f_tile = min(512, width), min(256, units)

        def forward(r):
            @pl.loop(0, width // tile)
            def _(j):
                cols = pl.ds(pl.multiple_of(j * tile, tile), tile)
                block = jnp.dot(hid_v[r], w_v[:, cols], preferred_element_type=F32)
                po[:, r, :, cols] = block.astype(BF16).reshape(n_y, -1, tile)

        def gathered(r):
            for key in gathers:
                if key[1] == r and key not in relayed:
                    gathers[key].wait_recv()

        loads["og"].wait()
        for item in near:
            gather(*item, 1)
        for c in range(PIECES_X):
            for k in order_x:
                cols = span(width, PIECES_X, c)
                target = dd.at[k, :, :, cols]
                go(remote(pg.at[at_x(k), :, :, cols], target, give_sem, k * PIECES_X + c, partner))
        go(remote(mom, mom_v.at[1], give_sem, MOM, partner))
        loads["w"].wait()
        loads["hid"].wait()
        forward(1)
        for item in far:
            gather(*item, 1)
        arrived(og_v.at[0, slot_me], give_sem, OG)
        for item in near:
            gather(*item, 0)

        @pl.loop(0, units // f_tile)
        def _(j):
            cols = pl.ds(pl.multiple_of(j * f_tile, f_tile), f_tile)
            wt_v[:, cols] = w_v[cols, :].T

        def back(a, b, r):
            wide = units // 2

            @pl.loop(0, 2)
            def _(j):
                cols = pl.ds(pl.multiple_of(j * wide, wide), wide)
                rows = og_v[r, pl.ds(a, b - a)].reshape(-1, width)
                block = jnp.dot(rows, wt_v[:, cols], preferred_element_type=F32).astype(BF16)
                part[pl.ds(a, b - a), :, r, :, cols] = block.reshape(b - a, 2, -1, wide)

        z_index = {key: i for i, key in enumerate(ring_items(n_z, 2 * PIECES_Z))}
        zs = {}

        def z_slot(k):
            return (k - shift) % n_z

        def z_send(s, h, d, r, c):
            k = z_slot(s * d)
            cols = span(units, PIECES_Z, c)
            i = r * PIECES_Z + c
            if d < arm(n_z, s, h):
                zs[s, h, d + 1, i].wait_recv()
                total = part[k, h, r, :, cols].astype(F32) + brecv[sign_at(s), h, d, r, :, cols].astype(F32)
                part[k, h, r, :, cols] = total.astype(BF16)
            target = brecv.at[sign_at(s), h, d - 1, r, :, cols]
            zs[s, h, d, i] = go(remote(part.at[k, h, r, :, cols], target, b_sem, z_index[s, h, d, i], to_z(s)))

        def z_wave(step, r):
            for long_arm in (True, False):
                for c in range(PIECES_Z):
                    for s in (1, -1):
                        h = 0 if (s > 0) == long_arm else 1
                        d = arm(n_z, s, h) - step
                        if d >= 1:
                            z_send(s, h, d, r, c)

        ends = {}

        def z_end(r):
            for c in range(PIECES_Z):
                i = r * PIECES_Z + c
                cols = span(units, PIECES_Z, c)
                for h in (0, 1):
                    total = part[z_slot(0), h, r, :, cols].astype(F32)
                    for s in (1, -1):
                        if arm(n_z, s, h) >= 1:
                            zs[s, h, 1, i].wait_recv()
                            total = total + brecv[sign_at(s), h, 0, r, :, cols].astype(F32)
                    fin[h, r, :, cols] = total
                xs[r, :, cols] = fin[1 - low, r, :, cols].astype(BF16)
                ends[i] = go(remote(xs.at[r, :, cols], xrv.at[r, :, cols], e_sem, i, pair))

        def grad_out(r):
            for c in range(PIECES_Z):
                i = r * PIECES_Z + c
                cols = span(units, PIECES_Z, c)
                ends[i].wait_recv()
                total = (fin[low, r, :, cols] + xrv[r, :, cols].astype(F32)).astype(BF16)
                if r == 1:
                    hg_o[:, cols] = total
                else:
                    hg_v[:, cols] = total
                    go(remote(hg_v.at[:, cols], hg_o.at[:, cols], h_sem, c, partner))

        cut = min(3, n_z)
        last = n_z // 2 - 1
        gathered(1)
        back(0, cut, 1)
        if n_z > 1:
            for s in (1, -1):

                @pl.when(lower_than[s])
                def _():
                    pl.semaphore_wait(z_sem.at[sign_at(s)], 1)

        z_wave(0, 1)
        for item in far:
            gather(*item, 0)
        if cut < n_z:
            back(cut, n_z, 1)
        arrived(hid_v.at[0], give_sem, HID)
        if last >= 1:
            z_wave(1, 1)
        gathered(0)
        back(0, cut, 0)
        z_wave(0, 0)
        forward(0)
        exchange = {}
        for o in range(1, n_y):
            exchange[o] = go(remote(po.at[lax.rem(y + o, n_y)], lrecv.at[o - 1], l_sem, o - 1, to_y(o)))
        if cut < n_z:
            back(cut, n_z, 0)
        for step in range(2, last + 1):
            z_wave(step, 1)
            z_wave(step - 1, 0)
        z_end(1)
        if last >= 1:
            z_wave(last, 0)
        z_end(0)
        grad_out(1)
        grad_out(0)

        total = po[y].astype(F32)
        for o in range(1, n_y):
            exchange[o].wait_recv()
            total = total + lrecv[o - 1].astype(F32)
        lay_v[...] = total[0].astype(BF16)
        lay_o[...] = total[1].astype(BF16)
        go(remote(lay_v, lay_o, give_sem, LAY, partner))

        for k in range(n_x):
            for h in (0, 1):
                for c in range(PIECES_X):
                    piece = out_o.at[at_x(k), h, :, span(width, PIECES_X, c)]
                    arrived(piece, pass_sem, (k * 2 + h) * PIECES_X + c)
        arrived(nm_o, give_sem, NM)
        for copy in sent:
            copy.wait_send()

    pl.when(core == 0)(x_program)
    pl.when(core == 1)(z_program)


def store(*refs):
    copies = [pltpu.make_async_copy(refs[i], refs[4 + i], refs[8].at[i]) for i in range(4)]
    for copy in copies:
        copy.start()
    for copy in copies:
        copy.wait()


def per_device(sizes, hidden, down_weight, out_grad, pseudo_grad, momentum):
    n_rep, n_dp, n_tp = sizes
    n_x, n_z = n_rep // 2, n_dp // 2
    tokens, units = hidden.shape[1:]
    width = down_weight.shape[1]
    rows = out_grad.shape[1]
    share = momentum.shape[0]
    owned = tokens // n_dp
    far_x, far_z = max(n_x // 2, 1), max(n_z // 2, 1)
    x_copies = max(len(ring_items(n_x, PIECES_X)), 1)
    z_copies = max(len(ring_items(n_z, 2 * PIECES_Z)), 1)
    near, far = gather_plan(n_tp)
    any_ref = pl.BlockSpec(memory_space=pl.ANY)
    vmem = pl.BlockSpec(memory_space=pltpu.VMEM)
    sem = pltpu.SemaphoreType.DMA
    results = pl.pallas_call(
        functools.partial(kernel, n_rep, n_dp, n_tp),
        out_shape=(
            pltpu.VMEM((rows, width), BF16),
            pltpu.VMEM((owned, units), BF16),
            pltpu.VMEM((share, width), F32),
            pltpu.VMEM((n_x, 2, share, width), BF16),
        ),
        in_specs=[any_ref] * 5,
        out_specs=(vmem,) * 4,
        scratch_shapes=[
            pltpu.VMEM((n_x, 2, share, width), BF16),
            pltpu.VMEM((n_x, 2, share, width), BF16),
            pltpu.VMEM((2, 2, far_x, share, width), BF16),
            pltpu.VMEM((2, share, width), F32),
            pltpu.VMEM((share, width), F32),
            pltpu.VMEM((2, tokens, units), BF16),
            pltpu.VMEM((units, width), BF16),
            pltpu.VMEM((width, units), BF16),
            pltpu.VMEM((2, n_tp, rows, width), BF16),
            pltpu.VMEM((n_tp, 2, rows, width), BF16),
            pltpu.VMEM((max(n_tp - 1, 1), 2, rows, width), BF16),
            pltpu.VMEM((rows, width), BF16),
            pltpu.VMEM((n_z, 2, 2, owned, units), BF16),
            pltpu.VMEM((2, 2, far_z, 2, owned, units), BF16),
            pltpu.VMEM((2, 2, owned, units), F32),
            pltpu.VMEM((2, owned, units), BF16),
            pltpu.VMEM((2, owned, units), BF16),
            pltpu.VMEM((owned, units), BF16),
            sem((max(n_x + 1, 3),)),
            sem((2, n_x * PIECES_X + 5)),
            sem((2, x_copies)),
            sem((2, x_copies)),
            sem((2, 2 * n_x * PIECES_X)),
            sem((2, max(2 * len(near + far), 1))),
            sem((2, max(n_tp - 1, 1))),
            sem((2, z_copies)),
            sem((2, 2 * PIECES_Z)),
            sem((2, PIECES_Z)),
            pltpu.SemaphoreType.REGULAR((2,)),
        ],
        compiler_params=pltpu.CompilerParams(collective_id=0, has_side_effects=True),
        name="step",
    )(
        hidden[0],
        down_weight,
        out_grad[0],
        pseudo_grad.reshape(n_x, 2, share, width),
        momentum,
    )
    lay, hg, nm, out = pl.pallas_call(
        store,
        out_shape=tuple(jax.ShapeDtypeStruct(r.shape, r.dtype) for r in results),
        in_specs=[vmem] * 4,
        out_specs=(any_ref,) * 4,
        scratch_shapes=[sem((4,))],
        compiler_params=pltpu.CompilerParams(vmem_limit_bytes=1 << 20),
        name="store",
    )(*results)
    return lay[None], hg[None], nm, out.reshape(down_weight.shape)


def solution(mesh):
    sizes = tuple(mesh.shape[axis] for axis in ("rep", "dp", "tp"))
    return jax.shard_map(
        functools.partial(per_device, sizes),
        mesh=mesh,
        in_specs=(
            P("rep", None, "tp"),
            P("tp", "dp"),
            P("rep", "tp", "dp"),
            P("rep", "tp", "dp"),
            P(("tp", "rep"), "dp"),
        ),
        out_specs=(
            P("rep", "tp", "dp"),
            P("rep", "dp", "tp"),
            P(("tp", "rep"), "dp"),
            P("tp", "dp"),
        ),
        check_vma=False,
    )
```
